512 devices in a mesh: node: 256 (over y_lo, x, z, core), tp: 2 (over y_hi).
Axes of the slice: x: 4, y: 4 (y_hi: 2, y_lo: 2; y = y_hi * 2 + y_lo), z: 16, core: 2. Of those that a mesh axis runs over, the one named last changes fastest.
Arguments:
- states: bfloat16 [256, 448, 4096], P('node', None, 'tp'), may hold values from -40 to 40
- weights: bfloat16 [256, 4096, 384], P('node', 'tp'), may hold values from -66 to 66
- norm_gain: float32 [4096], P('tp'), may hold values from 0.1 to 1.9
- cotangent: bfloat16 [256, 448, 128], P('node'), may hold values from -6 to 6
- round_index: int32 [1], replicated, may hold values from 0 to 999
Outputs:
- new_weights: bfloat16 [256, 4096, 384], P('node', 'tp')
The draws below stay inside these ranges and needn't reach their ends.
All inputs are finite; a program needn't handle non-finite values.
Results may differ from the reference program's by a relative error of at most 0.0095.
Values may be sent and summed in bfloat16 or wider, within the bound.
A program may use at most 64 MiB of HBM per device.

```python
import math
import jax
import jax.numpy as jnp
from jax import lax

D = 4096
HD = 128
TOK = 448
NODES = 256
N_NODE = 256


def draw_states(key, part):
    noise_key, jitter_key = jax.random.split(key, 2)
    position = jnp.arange(D, dtype=jnp.float32)
    jitter = jax.random.uniform(jitter_key, (NODES, 1, D), dtype=jnp.float32)
    scales = jnp.exp(jnp.log(10.0) * (position + jitter) / D)
    entries = jax.random.truncated_normal(noise_key, -4.0, 4.0, (NODES, TOK, D), jnp.float32)
    return (entries * scales).astype(jnp.bfloat16)


def draw_weights(key, part):
    base_key = jax.random.fold_in(key, 0)
    entries = jax.random.truncated_normal(base_key, -4.0, 4.0, (NODES, D, 3 * HD), jnp.float32)
    return entries.astype(jnp.bfloat16)


def level_of(stream_key, shape, cuts, smallest, high):
    factor_of, own = 1.0, jax.random.fold_in(stream_key, 6)
    for dim, parts in cuts:
        draws = jnp.exp(jax.random.uniform(jax.random.fold_in(own, dim), (parts,), jnp.float32, smallest / len(cuts), high / len(cuts)))
        factor_of = factor_of * jnp.repeat(draws, shape[dim] // parts).reshape([-1 if axis == dim else 1 for axis in range(len(shape))])
    return factor_of


def bell_draw(stream_key, shape, scale, reach, shards=(), kind=jnp.bfloat16):
    array = jax.random.normal(stream_key, shape, jnp.float32) * scale
    if len(shards) > 0:
        array = level_of(stream_key, shape, shards, -0.22, 0.18) * array
    return jnp.clip(array, min=-reach, max=reach).astype(kind)


def setup_inputs(seed: int = 0) -> dict:
    splits = jax.random.split(jax.random.key(seed), 6)
    return {
        "states": draw_states(jax.random.fold_in(splits[5], 71), 0),
        "weights": draw_weights(jax.random.fold_in(splits[5], 71), 0),
        "norm_gain": jnp.clip(1.0 + 0.18 * jax.random.normal(splits[2], (D,), jnp.float32), 0.1, 1.9),
        "cotangent": bell_draw(splits[3], (NODES, TOK, HD), 1.0, 6.0, ((0, 256),)),
        "round_index": jax.random.randint(splits[4], (1,), 0, 1000).astype(jnp.int32),
    }


rate = 0.5
norm_eps = 1e-05
step_eps = 1e-06

def contract(left, right, left_dim, right_dim):
    return lax.dot_general(left, right, (((left_dim,), (right_dim,)), ((), ())), preferred_element_type=jnp.float32)

def rope_tables(length, width):
    half_width = width // 2
    exponents = jnp.arange(half_width, dtype=jnp.float32) * (2.0 / width)
    frequency = jnp.exp(-jnp.log(jnp.float32(500000.0)) * exponents)
    angles = jnp.arange(length, dtype=jnp.float32)[:, None] * frequency[None, :]
    return (jnp.cos(angles), jnp.sin(angles))

def rotate(entries, cosine_table, sine_table):
    half_width = entries.shape[1] // 2
    leading = entries[:, :half_width]
    trailing = entries[:, half_width:]
    return jnp.concatenate([leading * cosine_table - trailing * sine_table, trailing * cosine_table + leading * sine_table], axis=1)

def unrotate(entries, cosine_table, sine_table):
    half_width = entries.shape[1] // 2
    leading = entries[:, :half_width]
    trailing = entries[:, half_width:]
    return jnp.concatenate([leading * cosine_table + trailing * sine_table, trailing * cosine_table - leading * sine_table], axis=1)

def attend_backward(projected, inv_rms, upstream):
    length = projected.shape[0]
    width = upstream.shape[1]
    cosine_table, sine_table = rope_tables(length, width)
    scaled = projected * inv_rms[:, None]
    queries = rotate(scaled[:, :width], cosine_table, sine_table).astype(jnp.bfloat16)
    keys = rotate(scaled[:, width:2 * width], cosine_table, sine_table).astype(jnp.bfloat16)
    values = scaled[:, 2 * width:].astype(jnp.bfloat16)
    scale_factor = 1.0 / math.sqrt(width)
    scores = contract(queries, keys, 1, 1) * scale_factor
    row_ids = jnp.arange(length, dtype=jnp.int32)
    causal = row_ids[None, :] <= row_ids[:, None]
    scores = jnp.where(causal, scores, -1e+30)
    peak = lax.optimization_barrier(jnp.max(scores, axis=1, keepdims=True))
    lifted = jnp.where(causal, jnp.exp(scores - peak), 0.0)
    probs = lifted / lax.optimization_barrier(jnp.sum(lifted, axis=1, keepdims=True))
    probs_low = probs.astype(jnp.bfloat16)
    attended = jnp.dot(probs_low, values, preferred_element_type=jnp.float32)
    row_dots = lax.optimization_barrier(jnp.sum(attended * upstream.astype(jnp.float32), axis=1))
    dvalues = contract(probs_low, upstream, 0, 0)
    dprobs = contract(upstream, values, 1, 1)
    dscores = (probs * (dprobs - row_dots[:, None]) * scale_factor).astype(jnp.bfloat16)
    dqueries = jnp.dot(dscores, keys, preferred_element_type=jnp.float32)
    dkeys = contract(dscores, queries, 0, 0)
    slope = jnp.concatenate([unrotate(dqueries, cosine_table, sine_table), unrotate(dkeys, cosine_table, sine_table), dvalues], axis=1)
    return (slope * inv_rms[:, None]).astype(jnp.bfloat16)

def take_step(weight_block, gradient, total, count):
    rms_value = jnp.sqrt(total / count + step_eps)
    return (weight_block.astype(jnp.float32) - rate * gradient / rms_value).astype(jnp.bfloat16)

def reference(states, weights, norm_gain, cotangent, round_index):

    def one_node(items):
        node_states, node_weights, upstream = items
        states_f32 = node_states.astype(jnp.float32)
        gained = (states_f32 * norm_gain).astype(jnp.bfloat16)
        projected = jnp.dot(gained, node_weights, preferred_element_type=jnp.float32) / math.sqrt(D)
        squares = lax.optimization_barrier(jnp.sum(states_f32 * states_f32, axis=1))
        inv_rms = lax.rsqrt(squares / D + norm_eps)
        slope = attend_backward(projected, inv_rms, upstream)
        gradient = contract(gained, slope, 0, 0)
        total = jnp.sum(gradient * gradient)
        return take_step(node_weights, gradient, total, D * 3 * HD)
    stepped = lax.map(one_node, (states, weights, cotangent))
    levels = N_NODE.bit_length() - 1
    offset = jnp.left_shift(jnp.int32(1), (round_index[0] % levels).astype(jnp.int32))
    partner = jnp.roll(stepped, offset, axis=0)
    return ((stepped.astype(jnp.float32) + partner.astype(jnp.float32)) * 0.5).astype(jnp.bfloat16)
```

```python
import functools
import math

import jax
import jax.numpy as jnp
import numpy as np
from jax import lax
from jax.experimental import pallas as pl
from jax.experimental.pallas import tpu as pltpu
from jax.sharding import PartitionSpec as P

MESH = pl.DeviceIdType.MESH

D = 4096
HD = 128
TOK = 448
PAD = 512
FEAT = D // 2
COLS = 3 * HD
W_PARTS = 4
ROW_PARTS = 2
CHUNKS = 16

rate = 0.5
norm_eps = 1e-05
step_eps = 1e-06


def angle_tables():
    half = HD // 2
    frequency = np.exp(-np.log(500000.0) * np.arange(half) * (2.0 / HD))
    frequency = np.concatenate([frequency, frequency])[None, :]
    coarse = (64.0 * np.arange(8))[:, None] * frequency
    fine = np.arange(64.0)[:, None] * frequency
    rows = [np.cos(coarse), np.sin(coarse), np.cos(fine), np.sin(fine)]
    return np.concatenate(rows, axis=0).astype(np.float32)


def dot(left, right, left_dim, right_dim):
    return lax.dot_general(
        left, right, (((left_dim,), (right_dim,)), ((), ())), preferred_element_type=jnp.float32
    )


def kernel(
    offset,
    nodes,
    states_hbm,
    weights_hbm,
    gain_hbm,
    cot_hbm,
    table_hbm,
    out_ref,
    x_buf,
    w_buf,
    gain_buf,
    cot_buf,
    table_buf,
    cos_buf,
    sin_buf,
    g_buf,
    gt_buf,
    p_own,
    p_send,
    p_recv,
    sq_own,
    sq_send,
    sq_recv,
    q_buf,
    k_buf,
    v_buf,
    dk_acc,
    dv_acc,
    slope_buf,
    grad_buf,
    step_buf,
    part_buf,
    tot_send,
    tot_recv,
    in_sems,
    x_sems,
    w_sems,
    p_send_sems,
    p_recv_sems,
    sq_sems,
    tot_sems,
    g_send_sems,
    g_recv_sems,
):
    me = lax.axis_index("node")
    half = lax.axis_index("tp")
    other = 1 - half
    target = lax.rem(me + offset, nodes)
    source = lax.rem(me + (nodes - offset), nodes)

    barrier = pltpu.get_barrier_semaphore()
    pl.semaphore_signal(barrier, inc=1, device_id={"tp": other}, device_id_type=MESH)
    pl.semaphore_signal(barrier, inc=1, device_id={"node": target}, device_id_type=MESH)
    pl.semaphore_signal(barrier, inc=1, device_id={"node": source}, device_id_type=MESH)

    w_rows = FEAT // W_PARTS
    x_rows = TOK // ROW_PARTS
    rows_of = FEAT // CHUNKS

    def w_copy(i):
        rows = pl.ds(i * w_rows, w_rows)
        return pltpu.make_async_copy(weights_hbm.at[0, rows], w_buf.at[rows], w_sems.at[i])

    def x_copy(i):
        rows = pl.ds(i * x_rows, x_rows)
        return pltpu.make_async_copy(states_hbm.at[0, rows], x_buf.at[rows], x_sems.at[i])

    gain_copy = pltpu.make_async_copy(gain_hbm, gain_buf, in_sems.at[0])
    cot_copy = pltpu.make_async_copy(cot_hbm.at[0], cot_buf.at[pl.ds(0, TOK)], in_sems.at[1])
    table_copy = pltpu.make_async_copy(table_hbm, table_buf, in_sems.at[2])

    gain_copy.start()
    x_copy(0).start()
    for i in range(W_PARTS):
        w_copy(i).start()
    for i in range(1, ROW_PARTS):
        x_copy(i).start()
    cot_copy.start()
    table_copy.start()

    g_buf[pl.ds(TOK, PAD - TOK), :] = jnp.zeros((PAD - TOK, FEAT), jnp.bfloat16)
    tail = jnp.zeros((PAD - TOK, HD), jnp.bfloat16)
    q_buf[pl.ds(TOK, PAD - TOK), :] = tail
    k_buf[pl.ds(TOK, PAD - TOK), :] = tail
    v_buf[pl.ds(TOK, PAD - TOK), :] = tail
    sq_own[pl.ds(TOK, PAD - TOK), :] = jnp.zeros((PAD - TOK, HD), jnp.float32)
    slope_buf[pl.ds(TOK, PAD - TOK), :] = jnp.zeros((PAD - TOK, COLS), jnp.bfloat16)

    def p_copy(i):
        rows = pl.ds(i * x_rows, x_rows)
        return pltpu.make_async_remote_copy(
            src_ref=p_send.at[rows],
            dst_ref=p_recv.at[rows],
            send_sem=p_send_sems.at[i],
            recv_sem=p_recv_sems.at[i],
            device_id={"tp": other},
            device_id_type=MESH,
        )

    sq_copy = pltpu.make_async_remote_copy(
        src_ref=sq_send,
        dst_ref=sq_recv,
        send_sem=sq_sems.at[0],
        recv_sem=sq_sems.at[1],
        device_id={"tp": other},
        device_id_type=MESH,
    )
    tot_copy = pltpu.make_async_remote_copy(
        src_ref=tot_send,
        dst_ref=tot_recv,
        send_sem=tot_sems.at[0],
        recv_sem=tot_sems.at[1],
        device_id={"tp": other},
        device_id_type=MESH,
    )

    def g_copy(i):
        rows = pl.ds(pl.multiple_of(i * rows_of, rows_of), rows_of)
        return pltpu.make_async_remote_copy(
            src_ref=step_buf.at[rows],
            dst_ref=part_buf.at[rows],
            send_sem=g_send_sems.at[i],
            recv_sem=g_recv_sems.at[i],
            device_id={"node": target},
            device_id_type=MESH,
        )

    gain_copy.wait()
    gain = gain_buf[...]
    for i in range(ROW_PARTS):
        rows = pl.ds(i * x_rows, x_rows)
        x_copy(i).wait()
        x = x_buf[rows, :].astype(jnp.float32)
        sq = jnp.sum(x * x, axis=1, keepdims=True)
        sq_own[rows, :] = jnp.broadcast_to(sq, (x_rows, HD))
        g_buf[rows, :] = (x * gain).astype(jnp.bfloat16)
        if i == 0:
            for j in range(W_PARTS):
                w_copy(j).wait()
        partial = dot(g_buf[rows, :], w_buf[...], 1, 0)
        p_own[rows, :] = partial
        p_send[rows, :] = partial.astype(jnp.bfloat16)
        if i == 0:
            pl.semaphore_wait(barrier, 3)
        p_copy(i).start()
    sq_send[...] = jnp.transpose(sq_own[...])[:8, :]
    sq_copy.start()

    cot_copy.wait()
    table_copy.wait()
    lane = lax.broadcasted_iota(jnp.int32, (64, HD), 1)
    sign = jnp.where(lane < HD // 2, -1.0, 1.0)
    cos_fine = table_buf[pl.ds(16, 64), :]
    sin_fine = table_buf[pl.ds(80, 64), :]
    for a in range(TOK // 64):
        cos_coarse = table_buf[pl.ds(a, 1), :]
        sin_coarse = table_buf[pl.ds(8 + a, 1), :]
        cos_buf[pl.ds(a * 64, 64), :] = cos_coarse * cos_fine - sin_coarse * sin_fine
        sin_buf[pl.ds(a * 64, 64), :] = (sin_coarse * cos_fine + cos_coarse * sin_fine) * sign

    def turn(c, carry):
        cols = pl.ds(pl.multiple_of(c * 256, 256), 256)
        gt_buf[cols, :] = jnp.transpose(g_buf[:, cols])
        return carry

    lax.fori_loop(0, FEAT // 256, turn, 0)

    cot_buf[pl.ds(TOK, PAD - TOK), :] = tail

    sq_copy.wait()
    squares = jnp.transpose(
        jnp.broadcast_to((sq_send[...] + sq_recv[...])[0:1, :], (HD, PAD))
    )
    inv_all = lax.rsqrt(squares[:TOK, :] / D + norm_eps)
    sq_own[pl.ds(0, TOK), :] = inv_all
    for i in range(ROW_PARTS):
        rows = pl.ds(i * x_rows, x_rows)
        p_copy(i).wait()
        inv = sq_own[rows, :]
        scale = inv * (1.0 / math.sqrt(D))
        cos = cos_buf[rows, :]
        sin = sin_buf[rows, :]

        def part(at):
            cols = pl.ds(at * HD, HD)
            return (p_own[rows, cols] + p_recv[rows, cols].astype(jnp.float32)) * scale

        q, k, v = part(0), part(1), part(2)
        q_buf[rows, :] = (q * cos + pltpu.roll(q, HD // 2, 1) * sin).astype(jnp.bfloat16)
        k_buf[rows, :] = (k * cos + pltpu.roll(k, HD // 2, 1) * sin).astype(jnp.bfloat16)
        v_buf[rows, :] = v.astype(jnp.bfloat16)

    dk_acc[...] = jnp.zeros_like(dk_acc)
    dv_acc[...] = jnp.zeros_like(dv_acc)
    factor = 1.0 / math.sqrt(HD)
    for b in range(4):
        height = 128 if b < 3 else TOK - 384
        width = 128 * (b + 1)
        rows = pl.ds(b * 128, height)
        keys = pl.ds(0, width)
        q = q_buf[rows, :]
        cot = cot_buf[rows, :]
        k = k_buf[keys, :]
        v = v_buf[keys, :]
        scores = dot(q, k, 1, 1) * factor
        row = lax.broadcasted_iota(jnp.int32, (height, width), 0) + b * 128
        col = lax.broadcasted_iota(jnp.int32, (height, width), 1)
        causal = col <= row
        scores = jnp.where(causal, scores, -1e30)
        peak = jnp.max(scores, axis=1, keepdims=True)
        lifted = jnp.where(causal, jnp.exp(scores - peak), 0.0)
        probs = lifted / jnp.sum(lifted, axis=1, keepdims=True)
        probs_low = probs.astype(jnp.bfloat16)
        dprobs = dot(cot, v, 1, 1)
        row_dots = jnp.sum(probs_low.astype(jnp.float32) * dprobs, axis=1, keepdims=True)
        dscores = (probs * (dprobs - row_dots) * factor).astype(jnp.bfloat16)
        dq = dot(dscores, k, 1, 0)
        dk_acc[keys, :] += dot(dscores, q, 0, 0)
        dv_acc[keys, :] += dot(probs_low, cot, 0, 0)
        cos = cos_buf[rows, :]
        sin = sin_buf[rows, :]
        inv = sq_own[rows, :]
        turned = dq * cos - pltpu.roll(dq, HD // 2, 1) * sin
        slope_buf[rows, pl.ds(0, HD)] = (turned * inv).astype(jnp.bfloat16)
    every = pl.ds(0, TOK)
    cos = cos_buf[every, :]
    sin = sin_buf[every, :]
    inv = sq_own[every, :]
    dk = dk_acc[every, :]
    turned = dk * cos - pltpu.roll(dk, HD // 2, 1) * sin
    slope_buf[every, pl.ds(HD, HD)] = (turned * inv).astype(jnp.bfloat16)
    slope_buf[every, pl.ds(2 * HD, HD)] = (dv_acc[every, :] * inv).astype(jnp.bfloat16)

    def gradient(c, so_far):
        rows = pl.ds(pl.multiple_of(c * 256, 256), 256)
        block = dot(gt_buf[rows, :], slope_buf[...], 1, 0)
        grad_buf[rows, :] = block
        return so_far + jnp.sum((block * block).reshape(32, 8, COLS), axis=0)

    squares_of = lax.fori_loop(0, FEAT // 256, gradient, jnp.zeros((8, COLS), jnp.float32))
    tot_send[...] = jnp.broadcast_to(jnp.sum(squares_of), (8, HD))
    tot_copy.start()
    tot_copy.wait()
    total = (tot_send[...] + tot_recv[...])[0:1, 0:1]
    pace = rate / jnp.sqrt(total / (D * COLS) + step_eps)

    def send(i, carry):
        rows = pl.ds(pl.multiple_of(i * rows_of, rows_of), rows_of)
        stepped = w_buf[rows, :].astype(jnp.float32) - grad_buf[rows, :] * pace
        step_buf[rows, :] = stepped.astype(jnp.bfloat16)
        g_copy(i).start()
        return carry

    lax.fori_loop(0, CHUNKS, send, 0)

    def receive(i, carry):
        rows = pl.ds(pl.multiple_of(i * rows_of, rows_of), rows_of)
        g_copy(i).wait_recv()
        mean = (step_buf[rows, :].astype(jnp.float32) + part_buf[rows, :].astype(jnp.float32)) * 0.5
        out_ref[0, rows, :] = mean.astype(jnp.bfloat16)
        return carry

    lax.fori_loop(0, CHUNKS, receive, 0)

    def finish(i, carry):
        g_copy(i).wait_send()
        return carry

    lax.fori_loop(0, CHUNKS, finish, 0)


def round_call(level, nodes):
    bf16, f32 = jnp.bfloat16, jnp.float32
    vmem, dma = pltpu.VMEM, pltpu.SemaphoreType.DMA
    return pl.pallas_call(
        functools.partial(kernel, 1 << level, nodes),
        out_shape=jax.ShapeDtypeStruct((1, FEAT, COLS), bf16),
        in_specs=[pl.BlockSpec(memory_space=pl.ANY)] * 5,
        out_specs=pl.BlockSpec(memory_space=pltpu.VMEM),
        scratch_shapes=[
            vmem((TOK, FEAT), bf16),
            vmem((FEAT, COLS), bf16),
            vmem((1, FEAT), f32),
            vmem((PAD, HD), bf16),
            vmem((144, HD), f32),
            vmem((TOK, HD), f32),
            vmem((TOK, HD), f32),
            vmem((PAD, FEAT), bf16),
            vmem((FEAT, PAD), bf16),
            vmem((TOK, COLS), f32),
            vmem((TOK, COLS), bf16),
            vmem((TOK, COLS), bf16),
            vmem((PAD, HD), f32),
            vmem((8, PAD), f32),
            vmem((8, PAD), f32),
            vmem((PAD, HD), bf16),
            vmem((PAD, HD), bf16),
            vmem((PAD, HD), bf16),
            vmem((PAD, HD), f32),
            vmem((PAD, HD), f32),
            vmem((PAD, COLS), bf16),
            vmem((FEAT, COLS), f32),
            vmem((FEAT, COLS), bf16),
            vmem((FEAT, COLS), bf16),
            vmem((8, HD), f32),
            vmem((8, HD), f32),
            dma((3,)),
            dma((ROW_PARTS,)),
            dma((W_PARTS,)),
            dma((ROW_PARTS,)),
            dma((ROW_PARTS,)),
            dma((2,)),
            dma((2,)),
            dma((CHUNKS,)),
            dma((CHUNKS,)),
        ],
        compiler_params=pltpu.CompilerParams(
            collective_id=level, has_side_effects=True, vmem_limit_bytes=40 << 20
        ),
        name=f"round_{level}",
    )


def per_device(states, weights, norm_gain, cotangent, round_index):
    nodes = lax.axis_size("node")
    levels = nodes.bit_length() - 1
    exponent = round_index[0] % levels
    table = jnp.asarray(angle_tables())
    return lax.switch(
        exponent,
        [round_call(level, nodes) for level in range(levels)],
        states,
        weights,
        norm_gain.reshape(1, FEAT),
        cotangent,
        table,
    )


def solution(mesh):
    return jax.shard_map(
        per_device,
        mesh=mesh,
        in_specs=(
            P("node", None, "tp"),
            P("node", "tp", None),
            P("tp"),
            P("node", None, None),
            P(),
        ),
        out_specs=P("node", "tp", None),
        check_vma=False,
    )
```

```python
import functools
import math

import jax
import jax.numpy as jnp
import numpy as np
from jax import lax
from jax.experimental import pallas as pl
from jax.experimental.pallas import tpu as pltpu
from jax.sharding import PartitionSpec as P

MESH = pl.DeviceIdType.MESH

D = 4096
HD = 128
TOK = 448
PAD = 512
FEAT = D // 2
COLS = 3 * HD
W_PARTS = 4
BLOCKS = ((0, 128), (128, 128), (256, 128), (384, 64))
CHUNKS = 16

rate = 0.5
norm_eps = 1e-05
step_eps = 1e-06


def angle_tables():
    half = HD // 2
    frequency = np.exp(-np.log(500000.0) * np.arange(half) * (2.0 / HD))
    frequency = np.concatenate([frequency, frequency])[None, :]
    coarse = (64.0 * np.arange(8))[:, None] * frequency
    fine = np.arange(64.0)[:, None] * frequency
    rows = [np.cos(coarse), np.sin(coarse), np.cos(fine), np.sin(fine)]
    return np.concatenate(rows, axis=0).astype(np.float32)


def along_z(node, by):
    depth = 32
    inner = lax.rem(node, depth)
    return node - inner + lax.rem(inner + (2 * by) % depth, depth)


def along_x(node, by):
    plane = 128
    inner = lax.rem(node, plane)
    return node - inner + lax.rem(inner + (32 * by) % plane, plane)


def route_of(level, nodes):
    if level == 2 and nodes >= 32:
        return 2, 2, 7, along_z
    if level == 3 and nodes >= 32:
        return 4, 2, 6, along_z
    if level == 5 and nodes == 256:
        return 4, 3, 1, along_x
    return 0, 1, 0, None


def dot(left, right, left_dim, right_dim):
    return lax.dot_general(
        left, right, (((left_dim,), (right_dim,)), ((), ())), preferred_element_type=jnp.float32
    )


def kernel(
    offset,
    nodes,
    route,
    states_hbm,
    weights_hbm,
    gain_hbm,
    cot_hbm,
    table_hbm,
    out_ref,
    x_buf,
    w_buf,
    gain_buf,
    cot_buf,
    table_buf,
    cos_buf,
    sin_buf,
    g_buf,
    gt_buf,
    p_own,
    p_send,
    p_recv,
    sq_own,
    sq_send,
    sq_recv,
    gram_buf,
    k_buf,
    v_buf,
    dk_acc,
    dv_acc,
    slope_buf,
    grad_buf,
    step_buf,
    part_buf,
    tot_send,
    tot_recv,
    in_sems,
    x_sems,
    w_sems,
    p_send_sems,
    p_recv_sems,
    sq_sems,
    tot_sems,
    g_send_sems,
    g_recv_sems,
    relay_buf,
    leg_send_sems,
    leg_recv_sems,
):
    me = lax.axis_index("node")
    half = lax.axis_index("tp")
    other = 1 - half
    target = lax.rem(me + offset, nodes)
    source = lax.rem(me + (nodes - offset), nodes)

    detour, legs, leap, along = route
    senders = [source]
    if detour:
        onward = along(me, -leap)
        last = lax.rem(along(me, (legs - 1) * leap) + offset, nodes)
        senders += [along(me, leap), along(source, -(legs - 1) * leap)]

    barrier = pltpu.get_barrier_semaphore()
    pl.semaphore_signal(barrier, inc=1, device_id={"tp": other}, device_id_type=MESH)
    for sender in senders:
        pl.semaphore_signal(barrier, inc=1, device_id={"node": sender}, device_id_type=MESH)

    w_rows = FEAT // W_PARTS
    rows_of = FEAT // CHUNKS

    def w_copy(i):
        rows = pl.ds(i * w_rows, w_rows)
        return pltpu.make_async_copy(weights_hbm.at[0, rows], w_buf.at[rows], w_sems.at[i])

    def x_copy(i, rows=None):
        rows = pl.ds(*BLOCKS[i]) if rows is None else rows
        return pltpu.make_async_copy(states_hbm.at[0, rows], x_buf.at[rows], x_sems.at[i])

    gain_copy = pltpu.make_async_copy(gain_hbm, gain_buf, in_sems.at[0])
    cot_copy = pltpu.make_async_copy(cot_hbm.at[0], cot_buf.at[pl.ds(0, TOK)], in_sems.at[1])
    table_copy = pltpu.make_async_copy(table_hbm, table_buf, in_sems.at[2])

    gain_copy.start()
    x_copy(0).start()
    for i in range(W_PARTS):
        w_copy(i).start()
    for i in range(1, len(BLOCKS)):
        x_copy(i).start()
    cot_copy.start()
    table_copy.start()

    x_buf[pl.ds(TOK, PAD - TOK), :] = jnp.zeros((PAD - TOK, FEAT), jnp.bfloat16)
    tail = jnp.zeros((PAD - TOK, HD), jnp.bfloat16)
    k_buf[pl.ds(TOK, PAD - TOK), :] = tail
    v_buf[pl.ds(TOK, PAD - TOK), :] = tail
    for n in range(3):
        slope_buf[pl.ds(n * PAD + TOK, PAD - TOK), :] = jnp.zeros((PAD - TOK, COLS), jnp.bfloat16)

    def p_copy(i, rows=None):
        rows = pl.ds(*BLOCKS[i]) if rows is None else rows
        return pltpu.make_async_remote_copy(
            src_ref=p_send.at[rows],
            dst_ref=p_recv.at[rows],
            send_sem=p_send_sems.at[i],
            recv_sem=p_recv_sems.at[i],
            device_id={"tp": other},
            device_id_type=MESH,
        )

    def sq_copy(i):
        return pltpu.make_async_remote_copy(
            src_ref=sq_send.at[i],
            dst_ref=sq_recv.at[i],
            send_sem=sq_sems.at[0, i],
            recv_sem=sq_sems.at[1, i],
            device_id={"tp": other},
            device_id_type=MESH,
        )

    tot_copy = pltpu.make_async_remote_copy(
        src_ref=tot_send,
        dst_ref=tot_recv,
        send_sem=tot_sems.at[0],
        recv_sem=tot_sems.at[1],
        device_id={"tp": other},
        device_id_type=MESH,
    )

    def g_copy(i):
        rows = pl.ds(pl.multiple_of(i * rows_of, rows_of), rows_of)
        return pltpu.make_async_remote_copy(
            src_ref=step_buf.at[rows],
            dst_ref=part_buf.at[rows],
            send_sem=g_send_sems.at[i],
            recv_sem=g_recv_sems.at[i],
            device_id={"node": target},
            device_id_type=MESH,
        )

    gain_copy.wait()
    gain = gain_buf[...]
    final = len(BLOCKS) - 1

    def project(i, carry):
        rows = pl.ds(pl.multiple_of(i * 128, 128), 128)

        @pl.when(i < final)
        def _():
            x_copy(i, rows).wait()

        @pl.when(i == final)
        def _():
            x_copy(final).wait()

        x = x_buf[rows, :].astype(jnp.float32)
        sq = jnp.sum(x * x, axis=1, keepdims=True)
        g_buf[rows, :] = (x * gain).astype(jnp.bfloat16)

        @pl.when(i == 0)
        def _():
            for j in range(W_PARTS):
                w_copy(j).wait()

        partial = dot(g_buf[rows, :], w_buf[...], 1, 0)
        p_own[rows, :] = partial
        p_send[rows, :] = partial.astype(jnp.bfloat16)
        sq_send[i] = jnp.transpose(jnp.broadcast_to(sq, (128, HD)))[:8, :]

        @pl.when(i == 0)
        def _():
            pl.semaphore_wait(barrier, 1 + len(senders))

        @pl.when(i < final)
        def _():
            p_copy(i, rows).start()

        @pl.when(i == final)
        def _():
            p_copy(final).start()

        sq_copy(i).start()
        return carry

    lax.fori_loop(0, len(BLOCKS), project, 0)

    cot_copy.wait()
    table_copy.wait()
    cot_buf[pl.ds(TOK, PAD - TOK), :] = tail
    lane = lax.broadcasted_iota(jnp.int32, (64, HD), 1)
    sign = jnp.where(lane < HD // 2, -1.0, 1.0)
    cos_fine = table_buf[pl.ds(16, 64), :]
    sin_fine = table_buf[pl.ds(80, 64), :]

    def tables(a, carry):
        rows = pl.ds(pl.multiple_of(a * 64, 64), 64)
        cos_coarse = table_buf[pl.ds(a, 1), :]
        sin_coarse = table_buf[pl.ds(8 + a, 1), :]
        cos_buf[rows, :] = cos_coarse * cos_fine - sin_coarse * sin_fine
        sin_buf[rows, :] = (sin_coarse * cos_fine + cos_coarse * sin_fine) * sign
        return carry

    lax.fori_loop(0, TOK // 64, tables, 0)

    def turn(c, carry):
        cols = pl.ds(pl.multiple_of(c * 256, 256), 256)
        gt_buf[cols, :] = jnp.transpose(g_buf[:, cols])
        return carry

    lax.fori_loop(0, FEAT // 256, turn, 0)

    def products(c, carry):
        rows = pl.ds(pl.multiple_of(c * 128, 128), 128)
        gram = dot(g_buf[rows, :], gt_buf[...], 1, 0)
        for level in range(3):
            short = gram.astype(jnp.bfloat16)
            gram_buf[rows, pl.ds(level * PAD, PAD)] = short
            gram = gram - short.astype(jnp.float32)
        return carry

    lax.fori_loop(0, PAD // 128, products, 0)

    dk_acc[...] = jnp.zeros_like(dk_acc)
    dv_acc[...] = jnp.zeros_like(dv_acc)
    factor = 1.0 / math.sqrt(HD)

    def put_slope(at, height, which, value):
        short = value.astype(jnp.bfloat16)
        for n in range(3):
            slope_buf[pl.ds(n * PAD + at, height), pl.ds(which * HD, HD)] = short

    for b, (at, height) in enumerate(BLOCKS):
        rows = pl.ds(at, height)
        sq_copy(b).wait()
        squares = jnp.transpose(
            jnp.broadcast_to((sq_send[b] + sq_recv[b])[0:1, :], (HD, HD))
        )
        inv = lax.rsqrt(squares[:height, :] / D + norm_eps)
        sq_own[rows, :] = inv
        scale = inv * (1.0 / math.sqrt(D))
        cos = cos_buf[rows, :]
        sin = sin_buf[rows, :]
        p_copy(b).wait()

        def part(n):
            cols = pl.ds(n * HD, HD)
            return (p_own[rows, cols] + p_recv[rows, cols].astype(jnp.float32)) * scale

        q, k, v = part(0), part(1), part(2)
        q = (q * cos + pltpu.roll(q, HD // 2, 1) * sin).astype(jnp.bfloat16)
        k_buf[rows, :] = (k * cos + pltpu.roll(k, HD // 2, 1) * sin).astype(jnp.bfloat16)
        v_buf[rows, :] = v.astype(jnp.bfloat16)

        width = 128 * (b + 1)
        keys = pl.ds(0, width)
        cot = cot_buf[rows, :]
        k = k_buf[keys, :]
        v = v_buf[keys, :]
        scores = dot(q, k, 1, 1) * factor
        row = lax.broadcasted_iota(jnp.int32, (height, width), 0) + at
        col = lax.broadcasted_iota(jnp.int32, (height, width), 1)
        causal = col <= row
        scores = jnp.where(causal, scores, -1e30)
        peak = jnp.max(scores, axis=1, keepdims=True)
        lifted = jnp.where(causal, jnp.exp(scores - peak), 0.0)
        probs = lifted / jnp.sum(lifted, axis=1, keepdims=True)
        probs_low = probs.astype(jnp.bfloat16)
        dprobs = dot(cot, v, 1, 1)
        row_dots = jnp.sum(probs_low.astype(jnp.float32) * dprobs, axis=1, keepdims=True)
        dscores = (probs * (dprobs - row_dots) * factor).astype(jnp.bfloat16)
        dq = dot(dscores, k, 1, 0)
        dk_acc[keys, :] += dot(dscores, q, 0, 0)
        dv_acc[keys, :] += dot(probs_low, cot, 0, 0)
        turned = dq * cos - pltpu.roll(dq, HD // 2, 1) * sin
        put_slope(at, height, 0, turned * inv)
    every = pl.ds(0, TOK)
    cos = cos_buf[every, :]
    sin = sin_buf[every, :]
    inv = sq_own[every, :]
    dk = dk_acc[every, :]
    turned = dk * cos - pltpu.roll(dk, HD // 2, 1) * sin
    put_slope(0, TOK, 1, turned * inv)
    put_slope(0, TOK, 2, dv_acc[every, :] * inv)
    def norms(c, so_far):
        rows = pl.ds(pl.multiple_of(c * 256, 256), 256)
        image = dot(gram_buf[rows, :], slope_buf[...], 1, 0)
        image = image * slope_buf[rows, :].astype(jnp.float32)
        return so_far + jnp.sum(image.reshape(32, 8, COLS), axis=0)

    total_of = lax.fori_loop(0, PAD // 256, norms, jnp.zeros((8, COLS), jnp.float32))
    tot_send[...] = jnp.broadcast_to(jnp.sum(total_of), (8, HD))
    tot_copy.start()

    def gradient(c, carry):
        rows = pl.ds(pl.multiple_of(c * 256, 256), 256)
        grad_buf[rows, :] = dot(gt_buf[rows, :], slope_buf[pl.ds(0, PAD), :], 1, 0)
        return carry

    lax.fori_loop(0, FEAT // 256, gradient, 0)
    tot_copy.wait()
    total = jnp.maximum(tot_send[...] + tot_recv[...], 0.0)[0:1, 0:1]
    pace = rate / jnp.sqrt(total / (D * COLS) + step_eps)
    def step(i):
        rows = pl.ds(pl.multiple_of(i * rows_of, rows_of), rows_of)
        stepped = w_buf[rows, :].astype(jnp.float32) - grad_buf[rows, :] * pace
        step_buf[rows, :] = stepped.astype(jnp.bfloat16)

    def leg_copy(leg, i):
        rows = pl.ds(pl.multiple_of(i * rows_of, rows_of), rows_of)
        first, closing = leg == 0, leg == legs - 1
        return pltpu.make_async_remote_copy(
            src_ref=step_buf.at[rows] if first else relay_buf.at[leg - 1, rows],
            dst_ref=part_buf.at[rows] if closing else relay_buf.at[leg, rows],
            send_sem=leg_send_sems.at[leg, i],
            recv_sem=g_recv_sems.at[i] if closing else leg_recv_sems.at[leg, i],
            device_id={"node": last if closing else onward},
            device_id_type=MESH,
        )

    def send_round(i, carry):
        step(i)
        leg_copy(0, i).start()
        return carry

    def send(i, carry):
        step(i)
        g_copy(i).start()
        return carry

    if detour:
        lax.fori_loop(0, detour, send_round, 0)
    lax.fori_loop(detour, CHUNKS, send, 0)

    for leg in range(1, legs):

        def relay(i, carry, leg=leg):
            leg_copy(leg - 1, i).wait_recv()
            leg_copy(leg, i).start()
            return carry

        lax.fori_loop(0, detour, relay, 0)

    def receive(i, carry):
        rows = pl.ds(pl.multiple_of(i * rows_of, rows_of), rows_of)
        g_copy(i).wait_recv()
        mean = (step_buf[rows, :].astype(jnp.float32) + part_buf[rows, :].astype(jnp.float32)) * 0.5
        out_ref[0, rows, :] = mean.astype(jnp.bfloat16)
        return carry

    lax.fori_loop(detour, CHUNKS, receive, 0)
    if detour:
        lax.fori_loop(0, detour, receive, 0)

    def finish(i, carry):
        g_copy(i).wait_send()
        return carry

    lax.fori_loop(detour, CHUNKS, finish, 0)
    for leg in range(legs if detour else 0):

        def finish_leg(i, carry, leg=leg):
            leg_copy(leg, i).wait_send()
            return carry

        lax.fori_loop(0, detour, finish_leg, 0)


def round_call(level, nodes):
    bf16, f32 = jnp.bfloat16, jnp.float32
    route = route_of(level, nodes)
    detour, legs = route[:2]
    vmem, dma = pltpu.VMEM, pltpu.SemaphoreType.DMA
    return pl.pallas_call(
        functools.partial(kernel, 1 << level, nodes, route),
        out_shape=jax.ShapeDtypeStruct((1, FEAT, COLS), bf16),
        in_specs=[pl.BlockSpec(memory_space=pl.ANY)] * 5,
        out_specs=pl.BlockSpec(memory_space=pltpu.VMEM),
        scratch_shapes=[
            vmem((PAD, FEAT), bf16),
            vmem((FEAT, COLS), bf16),
            vmem((1, FEAT), f32),
            vmem((PAD, HD), bf16),
            vmem((144, HD), f32),
            vmem((TOK, HD), f32),
            vmem((TOK, HD), f32),
            vmem((PAD, FEAT), bf16),
            vmem((FEAT, PAD), bf16),
            vmem((PAD, COLS), f32),
            vmem((PAD, COLS), bf16),
            vmem((PAD, COLS), bf16),
            vmem((PAD, HD), f32),
            vmem((len(BLOCKS), 8, HD), f32),
            vmem((len(BLOCKS), 8, HD), f32),
            vmem((PAD, 3 * PAD), bf16),
            vmem((PAD, HD), bf16),
            vmem((PAD, HD), bf16),
            vmem((PAD, HD), f32),
            vmem((PAD, HD), f32),
            vmem((3 * PAD, COLS), bf16),
            vmem((FEAT, COLS), f32),
            vmem((FEAT, COLS), bf16),
            vmem((FEAT, COLS), bf16),
            vmem((8, HD), f32),
            vmem((8, HD), f32),
            dma((3,)),
            dma((len(BLOCKS),)),
            dma((W_PARTS,)),
            dma((len(BLOCKS),)),
            dma((len(BLOCKS),)),
            dma((2, len(BLOCKS))),
            dma((2,)),
            dma((CHUNKS,)),
            dma((CHUNKS,)),
            vmem((max(legs - 1, 1), max(detour, 1) * FEAT // CHUNKS, COLS), bf16),
            dma((legs, max(detour, 1))),
            dma((max(legs - 1, 1), max(detour, 1))),
        ],
        compiler_params=pltpu.CompilerParams(
            collective_id=level, has_side_effects=True, vmem_limit_bytes=40 << 20
        ),
        name=f"round_{level}",
    )


def per_device(states, weights, norm_gain, cotangent, round_index):
    nodes = lax.axis_size("node")
    levels = nodes.bit_length() - 1
    exponent = round_index[0] % levels
    table = jnp.asarray(angle_tables())
    return lax.switch(
        exponent,
        [round_call(level, nodes) for level in range(levels)],
        states,
        weights,
        norm_gain.reshape(1, FEAT),
        cotangent,
        table,
    )


def solution(mesh):
    return jax.shard_map(
        per_device,
        mesh=mesh,
        in_specs=(
            P("node", None, "tp"),
            P("node", "tp", None),
            P("tp"),
            P("node", None, None),
            P(),
        ),
        out_specs=P("node", "tp", None),
        check_vma=False,
    )
```

```python
import functools
import math

import jax
import jax.numpy as jnp
import numpy as np
from jax import lax
from jax.experimental import pallas as pl
from jax.experimental.pallas import tpu as pltpu
from jax.sharding import PartitionSpec as P

MESH = pl.DeviceIdType.MESH

D = 4096
HD = 128
TOK = 448
PAD = 512
FEAT = D // 2
COLS = 3 * HD
W_PARTS = 4
BLOCKS = ((0, 128), (128, 128), (256, 128), (384, 64))

rate = 0.5
norm_eps = 1e-05
step_eps = 1e-06


def angle_tables():
    half = HD // 2
    frequency = np.exp(-np.log(500000.0) * np.arange(half) * (2.0 / HD))
    frequency = np.concatenate([frequency, frequency])[None, :]
    coarse = (64.0 * np.arange(8))[:, None] * frequency
    fine = np.arange(64.0)[:, None] * frequency
    rows = [np.cos(coarse), np.sin(coarse), np.cos(fine), np.sin(fine)]
    return np.concatenate(rows, axis=0).astype(np.float32)


def along_z(node, by):
    depth = 32
    inner = lax.rem(node, depth)
    return node - inner + lax.rem(inner + (2 * by) % depth, depth)


def along_x(node, by):
    plane = 128
    inner = lax.rem(node, plane)
    return node - inner + lax.rem(inner + (32 * by) % plane, plane)


def route_of(level, nodes):
    if level == 0:
        return 16, 2, 0, 1, 0, None
    if level == 2 and nodes >= 32:
        return 32, 1, 4, 2, 7, along_z
    if level == 3 and nodes >= 32:
        return 16, 0, 4, 2, 6, along_z
    if level == 4 and nodes >= 32:
        return 16, 0, 0, 1, 0, None
    if level == 5 and nodes == 256:
        return 16, 1, 4, 3, 1, along_x
    return 16, 1, 0, 1, 0, None


def dot(left, right, left_dim, right_dim):
    return lax.dot_general(
        left, right, (((left_dim,), (right_dim,)), ((), ())), preferred_element_type=jnp.float32
    )


def kernel(
    offset,
    nodes,
    route,
    states_hbm,
    weights_hbm,
    gain_hbm,
    cot_hbm,
    table_hbm,
    out_ref,
    x_buf,
    w_buf,
    gain_buf,
    cot_buf,
    table_buf,
    cos_buf,
    sin_buf,
    g_buf,
    gt_buf,
    p_own,
    p_send,
    p_recv,
    sq_own,
    sq_send,
    sq_recv,
    gram_buf,
    k_buf,
    v_buf,
    dk_acc,
    dv_acc,
    slope_buf,
    grad_buf,
    step_buf,
    part_buf,
    tot_send,
    tot_recv,
    in_sems,
    x_sems,
    w_sems,
    p_send_sems,
    p_recv_sems,
    sq_sems,
    tot_sems,
    g_send_sems,
    g_recv_sems,
    relay_buf,
    leg_send_sems,
    leg_recv_sems,
    old_buf,
    short_buf,
    slant_buf,
    pace_send,
    pace_recv,
    early_sems,
):
    me = lax.axis_index("node")
    half = lax.axis_index("tp")
    other = 1 - half
    target = lax.rem(me + offset, nodes)
    source = lax.rem(me + (nodes - offset), nodes)

    chunks, early, detour, legs, leap, along = route
    senders = [source]
    if detour:
        onward = along(me, -leap)
        last = lax.rem(along(me, (legs - 1) * leap) + offset, nodes)
        senders += [along(me, leap), along(source, -(legs - 1) * leap)]

    barrier = pltpu.get_barrier_semaphore()
    pl.semaphore_signal(barrier, inc=1, device_id={"tp": other}, device_id_type=MESH)
    for sender in senders:
        pl.semaphore_signal(barrier, inc=1, device_id={"node": sender}, device_id_type=MESH)

    w_rows = FEAT // W_PARTS
    rows_of = FEAT // chunks
    fresh = early * rows_of
    late = pl.ds(FEAT - fresh, fresh)
    regular = chunks - early

    def w_copy(i):
        rows = pl.ds(i * w_rows, w_rows)
        return pltpu.make_async_copy(weights_hbm.at[0, rows], w_buf.at[rows], w_sems.at[i])

    def x_copy(i, rows=None):
        rows = pl.ds(*BLOCKS[i]) if rows is None else rows
        return pltpu.make_async_copy(states_hbm.at[0, rows], x_buf.at[rows], x_sems.at[i])

    gain_copy = pltpu.make_async_copy(gain_hbm, gain_buf, in_sems.at[0])
    cot_copy = pltpu.make_async_copy(cot_hbm.at[0], cot_buf.at[pl.ds(0, TOK)], in_sems.at[1])
    table_copy = pltpu.make_async_copy(table_hbm, table_buf, in_sems.at[2])

    gain_copy.start()
    x_copy(0).start()
    for i in range(W_PARTS):
        w_copy(i).start()
    for i in range(1, len(BLOCKS)):
        x_copy(i).start()
    cot_copy.start()
    table_copy.start()

    x_buf[pl.ds(TOK, PAD - TOK), :] = jnp.zeros((PAD - TOK, FEAT), jnp.bfloat16)
    tail = jnp.zeros((PAD - TOK, HD), jnp.bfloat16)
    k_buf[pl.ds(TOK, PAD - TOK), :] = tail
    v_buf[pl.ds(TOK, PAD - TOK), :] = tail
    for n in range(3):
        slope_buf[pl.ds(n * PAD + TOK, PAD - TOK), :] = jnp.zeros((PAD - TOK, COLS), jnp.bfloat16)

    def p_copy(i, rows=None):
        rows = pl.ds(*BLOCKS[i]) if rows is None else rows
        return pltpu.make_async_remote_copy(
            src_ref=p_send.at[rows],
            dst_ref=p_recv.at[rows],
            send_sem=p_send_sems.at[i],
            recv_sem=p_recv_sems.at[i],
            device_id={"tp": other},
            device_id_type=MESH,
        )

    def sq_copy(i):
        return pltpu.make_async_remote_copy(
            src_ref=sq_send.at[i],
            dst_ref=sq_recv.at[i],
            send_sem=sq_sems.at[0, i],
            recv_sem=sq_sems.at[1, i],
            device_id={"tp": other},
            device_id_type=MESH,
        )

    tot_copy = pltpu.make_async_remote_copy(
        src_ref=tot_send,
        dst_ref=tot_recv,
        send_sem=tot_sems.at[0],
        recv_sem=tot_sems.at[1],
        device_id={"tp": other},
        device_id_type=MESH,
    )

    def early_copy(n):
        pairs = ((w_buf.at[late], old_buf), (short_buf, slant_buf), (pace_send, pace_recv))
        return pltpu.make_async_remote_copy(
            src_ref=pairs[n][0],
            dst_ref=pairs[n][1],
            send_sem=early_sems.at[0, n],
            recv_sem=early_sems.at[1, n],
            device_id={"node": target},
            device_id_type=MESH,
        )

    def g_copy(i):
        rows = pl.ds(pl.multiple_of(i * rows_of, rows_of), rows_of)
        return pltpu.make_async_remote_copy(
            src_ref=step_buf.at[rows],
            dst_ref=part_buf.at[rows],
            send_sem=g_send_sems.at[i],
            recv_sem=g_recv_sems.at[i],
            device_id={"node": target},
            device_id_type=MESH,
        )

    gain_copy.wait()
    gain = gain_buf[...]
    final = len(BLOCKS) - 1

    def project(i, carry):
        rows = pl.ds(pl.multiple_of(i * 128, 128), 128)

        @pl.when(i < final)
        def _():
            x_copy(i, rows).wait()

        @pl.when(i == final)
        def _():
            x_copy(final).wait()

        x = x_buf[rows, :].astype(jnp.float32)
        sq = jnp.sum(x * x, axis=1, keepdims=True)
        g_buf[rows, :] = (x * gain).astype(jnp.bfloat16)

        @pl.when(i == 0)
        def _():
            for j in range(W_PARTS):
                w_copy(j).wait()

        partial = dot(g_buf[rows, :], w_buf[...], 1, 0)
        p_own[rows, :] = partial
        p_send[rows, :] = partial.astype(jnp.bfloat16)
        sq_send[i] = jnp.transpose(jnp.broadcast_to(sq, (128, HD)))[:8, :]

        @pl.when(i == 0)
        def _():
            pl.semaphore_wait(barrier, 1 + len(senders))

        @pl.when(i < final)
        def _():
            p_copy(i, rows).start()

        @pl.when(i == final)
        def _():
            p_copy(final).start()

        sq_copy(i).start()
        return carry

    lax.fori_loop(0, len(BLOCKS), project, 0)

    cot_copy.wait()
    table_copy.wait()
    cot_buf[pl.ds(TOK, PAD - TOK), :] = tail
    lane = lax.broadcasted_iota(jnp.int32, (64, HD), 1)
    sign = jnp.where(lane < HD // 2, -1.0, 1.0)
    cos_fine = table_buf[pl.ds(16, 64), :]
    sin_fine = table_buf[pl.ds(80, 64), :]

    def tables(a, carry):
        rows = pl.ds(pl.multiple_of(a * 64, 64), 64)
        cos_coarse = table_buf[pl.ds(a, 1), :]
        sin_coarse = table_buf[pl.ds(8 + a, 1), :]
        cos_buf[rows, :] = cos_coarse * cos_fine - sin_coarse * sin_fine
        sin_buf[rows, :] = (sin_coarse * cos_fine + cos_coarse * sin_fine) * sign
        return carry

    lax.fori_loop(0, TOK // 64, tables, 0)

    def turn(c, carry):
        cols = pl.ds(pl.multiple_of(c * 256, 256), 256)
        gt_buf[cols, :] = jnp.transpose(g_buf[:, cols])
        return carry

    lax.fori_loop(0, FEAT // 256, turn, 0)

    def products(c, carry):
        rows = pl.ds(pl.multiple_of(c * 128, 128), 128)
        gram = dot(g_buf[rows, :], gt_buf[...], 1, 0)
        for level in range(3):
            short = gram.astype(jnp.bfloat16)
            gram_buf[rows, pl.ds(level * PAD, PAD)] = short
            gram = gram - short.astype(jnp.float32)
        return carry

    lax.fori_loop(0, PAD // 128, products, 0)

    dk_acc[...] = jnp.zeros_like(dk_acc)
    dv_acc[...] = jnp.zeros_like(dv_acc)
    factor = 1.0 / math.sqrt(HD)

    def put_slope(at, height, which, value):
        short = value.astype(jnp.bfloat16)
        for n in range(3):
            slope_buf[pl.ds(n * PAD + at, height), pl.ds(which * HD, HD)] = short

    for b, (at, height) in enumerate(BLOCKS):
        rows = pl.ds(at, height)
        sq_copy(b).wait()
        squares = jnp.transpose(
            jnp.broadcast_to((sq_send[b] + sq_recv[b])[0:1, :], (HD, HD))
        )
        inv = lax.rsqrt(squares[:height, :] / D + norm_eps)
        sq_own[rows, :] = inv
        scale = inv * (1.0 / math.sqrt(D))
        cos = cos_buf[rows, :]
        sin = sin_buf[rows, :]
        p_copy(b).wait()
        if early and b == final:
            early_copy(0).start()

        def part(n):
            cols = pl.ds(n * HD, HD)
            return (p_own[rows, cols] + p_recv[rows, cols].astype(jnp.float32)) * scale

        q, k, v = part(0), part(1), part(2)
        q = (q * cos + pltpu.roll(q, HD // 2, 1) * sin).astype(jnp.bfloat16)
        k_buf[rows, :] = (k * cos + pltpu.roll(k, HD // 2, 1) * sin).astype(jnp.bfloat16)
        v_buf[rows, :] = v.astype(jnp.bfloat16)

        width = 128 * (b + 1)
        keys = pl.ds(0, width)
        cot = cot_buf[rows, :]
        k = k_buf[keys, :]
        v = v_buf[keys, :]
        scores = dot(q, k, 1, 1) * factor
        row = lax.broadcasted_iota(jnp.int32, (height, width), 0) + at
        col = lax.broadcasted_iota(jnp.int32, (height, width), 1)
        causal = col <= row
        scores = jnp.where(causal, scores, -1e30)
        peak = jnp.max(scores, axis=1, keepdims=True)
        lifted = jnp.where(causal, jnp.exp(scores - peak), 0.0)
        probs = lifted / jnp.sum(lifted, axis=1, keepdims=True)
        probs_low = probs.astype(jnp.bfloat16)
        dprobs = dot(cot, v, 1, 1)
        row_dots = jnp.sum(probs_low.astype(jnp.float32) * dprobs, axis=1, keepdims=True)
        dscores = (probs * (dprobs - row_dots) * factor).astype(jnp.bfloat16)
        dq = dot(dscores, k, 1, 0)
        dk_acc[keys, :] += dot(dscores, q, 0, 0)
        dv_acc[keys, :] += dot(probs_low, cot, 0, 0)
        turned = dq * cos - pltpu.roll(dq, HD // 2, 1) * sin
        put_slope(at, height, 0, turned * inv)
    every = pl.ds(0, TOK)
    cos = cos_buf[every, :]
    sin = sin_buf[every, :]
    inv = sq_own[every, :]
    dk = dk_acc[every, :]
    turned = dk * cos - pltpu.roll(dk, HD // 2, 1) * sin
    put_slope(0, TOK, 1, turned * inv)
    put_slope(0, TOK, 2, dv_acc[every, :] * inv)
    if early:
        block = dot(gt_buf[late, :], slope_buf[pl.ds(0, PAD), :], 1, 0)
        short_buf[...] = block.astype(jnp.bfloat16)
        early_copy(1).start()

    def norms(c, so_far):
        rows = pl.ds(pl.multiple_of(c * 256, 256), 256)
        image = dot(gram_buf[rows, :], slope_buf[...], 1, 0)
        image = image * slope_buf[rows, :].astype(jnp.float32)
        return so_far + jnp.sum(image.reshape(32, 8, COLS), axis=0)

    total_of = lax.fori_loop(0, PAD // 256, norms, jnp.zeros((8, COLS), jnp.float32))
    tot_send[...] = jnp.broadcast_to(jnp.sum(total_of), (8, HD))
    tot_copy.start()

    def gradient(c, carry):
        rows = pl.ds(pl.multiple_of(c * 256, 256), 256)
        grad_buf[rows, :] = dot(gt_buf[rows, :], slope_buf[pl.ds(0, PAD), :], 1, 0)
        return carry

    lax.fori_loop(0, FEAT // 256, gradient, 0)
    tot_copy.wait()
    total = jnp.maximum(tot_send[...] + tot_recv[...], 0.0)[0:1, 0:1]
    pace = rate / jnp.sqrt(total / (D * COLS) + step_eps)
    if early:
        pace_send[...] = jnp.broadcast_to(pace, (8, HD))
        early_copy(2).start()

    def step(i):
        rows = pl.ds(pl.multiple_of(i * rows_of, rows_of), rows_of)
        stepped = w_buf[rows, :].astype(jnp.float32) - grad_buf[rows, :] * pace
        step_buf[rows, :] = stepped.astype(jnp.bfloat16)

    def leg_copy(leg, i):
        rows = pl.ds(pl.multiple_of(i * rows_of, rows_of), rows_of)
        first, closing = leg == 0, leg == legs - 1
        return pltpu.make_async_remote_copy(
            src_ref=step_buf.at[rows] if first else relay_buf.at[leg - 1, rows],
            dst_ref=part_buf.at[rows] if closing else relay_buf.at[leg, rows],
            send_sem=leg_send_sems.at[leg, i],
            recv_sem=g_recv_sems.at[i] if closing else leg_recv_sems.at[leg, i],
            device_id={"node": last if closing else onward},
            device_id_type=MESH,
        )

    def send_round(i, carry):
        step(i)
        leg_copy(0, i).start()
        return carry

    def send(i, carry):
        step(i)
        g_copy(i).start()
        return carry

    if detour:
        lax.fori_loop(0, detour, send_round, 0)
    lax.fori_loop(detour, regular, send, 0)

    for leg in range(1, legs):

        def relay(i, carry, leg=leg):
            leg_copy(leg - 1, i).wait_recv()
            leg_copy(leg, i).start()
            return carry

        lax.fori_loop(0, detour, relay, 0)

    def receive(i, carry):
        rows = pl.ds(pl.multiple_of(i * rows_of, rows_of), rows_of)
        g_copy(i).wait_recv()
        mean = (step_buf[rows, :].astype(jnp.float32) + part_buf[rows, :].astype(jnp.float32)) * 0.5
        out_ref[0, rows, :] = mean.astype(jnp.bfloat16)
        return carry

    if early:
        for n in range(3):
            early_copy(n).wait()
        own = w_buf[late, :].astype(jnp.float32) - grad_buf[late, :] * pace
        theirs = old_buf[...].astype(jnp.float32) - slant_buf[...].astype(jnp.float32) * pace_recv[0:1, 0:1]
        own, theirs = (side.astype(jnp.bfloat16).astype(jnp.float32) for side in (own, theirs))
        out_ref[0, late, :] = ((own + theirs) * 0.5).astype(jnp.bfloat16)
    lax.fori_loop(detour, regular, receive, 0)
    if detour:
        lax.fori_loop(0, detour, receive, 0)

    def finish(i, carry):
        g_copy(i).wait_send()
        return carry

    lax.fori_loop(detour, regular, finish, 0)
    for leg in range(legs if detour else 0):

        def finish_leg(i, carry, leg=leg):
            leg_copy(leg, i).wait_send()
            return carry

        lax.fori_loop(0, detour, finish_leg, 0)


def round_call(level, nodes):
    bf16, f32 = jnp.bfloat16, jnp.float32
    route = route_of(level, nodes)
    chunks, early, detour, legs = route[:4]
    fresh = max(early, 1) * FEAT // chunks
    vmem, dma = pltpu.VMEM, pltpu.SemaphoreType.DMA
    return pl.pallas_call(
        functools.partial(kernel, 1 << level, nodes, route),
        out_shape=jax.ShapeDtypeStruct((1, FEAT, COLS), bf16),
        in_specs=[pl.BlockSpec(memory_space=pl.ANY)] * 5,
        out_specs=pl.BlockSpec(memory_space=pltpu.VMEM),
        scratch_shapes=[
            vmem((PAD, FEAT), bf16),
            vmem((FEAT, COLS), bf16),
            vmem((1, FEAT), f32),
            vmem((PAD, HD), bf16),
            vmem((144, HD), f32),
            vmem((TOK, HD), f32),
            vmem((TOK, HD), f32),
            vmem((PAD, FEAT), bf16),
            vmem((FEAT, PAD), bf16),
            vmem((PAD, COLS), f32),
            vmem((PAD, COLS), bf16),
            vmem((PAD, COLS), bf16),
            vmem((PAD, HD), f32),
            vmem((len(BLOCKS), 8, HD), f32),
            vmem((len(BLOCKS), 8, HD), f32),
            vmem((PAD, 3 * PAD), bf16),
            vmem((PAD, HD), bf16),
            vmem((PAD, HD), bf16),
            vmem((PAD, HD), f32),
            vmem((PAD, HD), f32),
            vmem((3 * PAD, COLS), bf16),
            vmem((FEAT, COLS), f32),
            vmem((FEAT, COLS), bf16),
            vmem((FEAT, COLS), bf16),
            vmem((8, HD), f32),
            vmem((8, HD), f32),
            dma((3,)),
            dma((len(BLOCKS),)),
            dma((W_PARTS,)),
            dma((len(BLOCKS),)),
            dma((len(BLOCKS),)),
            dma((2, len(BLOCKS))),
            dma((2,)),
            dma((chunks,)),
            dma((chunks,)),
            vmem((max(legs - 1, 1), max(detour, 1) * FEAT // chunks, COLS), bf16),
            dma((legs, max(detour, 1))),
            dma((max(legs - 1, 1), max(detour, 1))),
            vmem((fresh, COLS), bf16),
            vmem((fresh, COLS), bf16),
            vmem((fresh, COLS), bf16),
            vmem((8, HD), f32),
            vmem((8, HD), f32),
            dma((2, 3)),
        ],
        compiler_params=pltpu.CompilerParams(
            collective_id=level, has_side_effects=True, vmem_limit_bytes=40 << 20
        ),
        name=f"round_{level}",
    )


def per_device(states, weights, norm_gain, cotangent, round_index):
    nodes = lax.axis_size("node")
    levels = nodes.bit_length() - 1
    exponent = round_index[0] % levels
    table = jnp.asarray(angle_tables())
    return lax.switch(
        exponent,
        [round_call(level, nodes) for level in range(levels)],
        states,
        weights,
        norm_gain.reshape(1, FEAT),
        cotangent,
        table,
    )


def solution(mesh):
    return jax.shard_map(
        per_device,
        mesh=mesh,
        in_specs=(
            P("node", None, "tp"),
            P("node", "tp", None),
            P("tp"),
            P("node", None, None),
            P(),
        ),
        out_specs=P("node", "tp", None),
        check_vma=False,
    )
```

```python
import functools
import math

import jax
import jax.numpy as jnp
import numpy as np
from jax import lax
from jax.experimental import pallas as pl
from jax.experimental.pallas import tpu as pltpu
from jax.sharding import PartitionSpec as P

MESH = pl.DeviceIdType.MESH

D = 4096
HD = 128
TOK = 448
PAD = 512
FEAT = D // 2
COLS = 3 * HD
W_PARTS = 4
BLOCKS = ((0, 128), (128, 128), (256, 128), (384, 64))

rate = 0.5
norm_eps = 1e-05
step_eps = 1e-06


def angle_tables():
    half = HD // 2
    frequency = np.exp(-np.log(500000.0) * np.arange(half) * (2.0 / HD))
    frequency = np.concatenate([frequency, frequency])[None, :]
    coarse = (64.0 * np.arange(8))[:, None] * frequency
    fine = np.arange(64.0)[:, None] * frequency
    rows = [np.cos(coarse), np.sin(coarse), np.cos(fine), np.sin(fine)]
    return np.concatenate(rows, axis=0).astype(np.float32)


def along_z(node, by):
    depth = 32
    inner = lax.rem(node, depth)
    return node - inner + lax.rem(inner + (2 * by) % depth, depth)


def along_x(node, by):
    plane = 128
    inner = lax.rem(node, plane)
    return node - inner + lax.rem(inner + (32 * by) % plane, plane)


def route_of(level, nodes):
    if level == 0:
        return 16, 3, 0, 1, 0, None
    if level == 2 and nodes >= 32:
        return 32, 1, 4, 2, 7, along_z
    if level == 3 and nodes >= 32:
        return 16, 0, 4, 2, 6, along_z
    if level == 4 and nodes >= 32:
        return 16, 0, 0, 1, 0, None
    if level == 5 and nodes == 256:
        return 16, 1, 4, 3, 1, along_x
    return 32, 3, 0, 1, 0, None


def dot(left, right, left_dim, right_dim):
    return lax.dot_general(
        left, right, (((left_dim,), (right_dim,)), ((), ())), preferred_element_type=jnp.float32
    )


def kernel(
    offset,
    nodes,
    route,
    states_hbm,
    weights_hbm,
    gain_hbm,
    cot_hbm,
    table_hbm,
    out_ref,
    x_buf,
    w_buf,
    gain_buf,
    cot_buf,
    table_buf,
    cos_buf,
    sin_buf,
    g_buf,
    gt_buf,
    p_own,
    p_send,
    p_recv,
    sq_own,
    sq_send,
    sq_recv,
    gram_buf,
    k_buf,
    v_buf,
    dk_acc,
    dv_acc,
    slope_buf,
    grad_buf,
    step_buf,
    part_buf,
    tot_send,
    tot_recv,
    in_sems,
    x_sems,
    w_sems,
    p_send_sems,
    p_recv_sems,
    sq_sems,
    tot_sems,
    g_send_sems,
    g_recv_sems,
    relay_buf,
    leg_send_sems,
    leg_recv_sems,
    old_buf,
    short_buf,
    slant_buf,
    pace_send,
    pace_recv,
    early_sems,
):
    me = lax.axis_index("node")
    half = lax.axis_index("tp")
    other = 1 - half
    target = lax.rem(me + offset, nodes)
    source = lax.rem(me + (nodes - offset), nodes)

    chunks, early, detour, legs, leap, along = route
    senders = [source]
    if detour:
        onward = along(me, -leap)
        last = lax.rem(along(me, (legs - 1) * leap) + offset, nodes)
        senders += [along(me, leap), along(source, -(legs - 1) * leap)]

    barrier = pltpu.get_barrier_semaphore()
    pl.semaphore_signal(barrier, inc=1, device_id={"tp": other}, device_id_type=MESH)
    for sender in senders:
        pl.semaphore_signal(barrier, inc=1, device_id={"node": sender}, device_id_type=MESH)

    w_rows = FEAT // W_PARTS
    rows_of = FEAT // chunks
    fresh = early * rows_of
    late = pl.ds(FEAT - fresh, fresh)
    regular = chunks - early

    def w_copy(i):
        rows = pl.ds(i * w_rows, w_rows)
        return pltpu.make_async_copy(weights_hbm.at[0, rows], w_buf.at[rows], w_sems.at[i])

    def x_copy(i, rows=None):
        rows = pl.ds(*BLOCKS[i]) if rows is None else rows
        return pltpu.make_async_copy(states_hbm.at[0, rows], x_buf.at[rows], x_sems.at[i])

    gain_copy = pltpu.make_async_copy(gain_hbm, gain_buf, in_sems.at[0])
    cot_copy = pltpu.make_async_copy(cot_hbm.at[0], cot_buf.at[pl.ds(0, TOK)], in_sems.at[1])
    table_copy = pltpu.make_async_copy(table_hbm, table_buf, in_sems.at[2])

    gain_copy.start()
    x_copy(0).start()
    for i in range(W_PARTS):
        w_copy(i).start()
    for i in range(1, len(BLOCKS)):
        x_copy(i).start()
    cot_copy.start()
    table_copy.start()

    x_buf[pl.ds(TOK, PAD - TOK), :] = jnp.zeros((PAD - TOK, FEAT), jnp.bfloat16)
    tail = jnp.zeros((PAD - TOK, HD), jnp.bfloat16)
    k_buf[pl.ds(TOK, PAD - TOK), :] = tail
    v_buf[pl.ds(TOK, PAD - TOK), :] = tail
    for n in range(3):
        slope_buf[pl.ds(n * PAD + TOK, PAD - TOK), :] = jnp.zeros((PAD - TOK, COLS), jnp.bfloat16)

    def p_copy(i, rows=None):
        rows = pl.ds(*BLOCKS[i]) if rows is None else rows
        return pltpu.make_async_remote_copy(
            src_ref=p_send.at[rows],
            dst_ref=p_recv.at[rows],
            send_sem=p_send_sems.at[i],
            recv_sem=p_recv_sems.at[i],
            device_id={"tp": other},
            device_id_type=MESH,
        )

    def sq_copy(i):
        return pltpu.make_async_remote_copy(
            src_ref=sq_send.at[i],
            dst_ref=sq_recv.at[i],
            send_sem=sq_sems.at[0, i],
            recv_sem=sq_sems.at[1, i],
            device_id={"tp": other},
            device_id_type=MESH,
        )

    tot_copy = pltpu.make_async_remote_copy(
        src_ref=tot_send,
        dst_ref=tot_recv,
        send_sem=tot_sems.at[0],
        recv_sem=tot_sems.at[1],
        device_id={"tp": other},
        device_id_type=MESH,
    )

    def early_copy(n):
        pairs = ((w_buf.at[late], old_buf), (short_buf, slant_buf), (pace_send, pace_recv))
        return pltpu.make_async_remote_copy(
            src_ref=pairs[n][0],
            dst_ref=pairs[n][1],
            send_sem=early_sems.at[0, n],
            recv_sem=early_sems.at[1, n],
            device_id={"node": target},
            device_id_type=MESH,
        )

    def g_copy(i):
        rows = pl.ds(pl.multiple_of(i * rows_of, rows_of), rows_of)
        return pltpu.make_async_remote_copy(
            src_ref=step_buf.at[rows],
            dst_ref=part_buf.at[rows],
            send_sem=g_send_sems.at[i],
            recv_sem=g_recv_sems.at[i],
            device_id={"node": target},
            device_id_type=MESH,
        )

    gain_copy.wait()
    gain = gain_buf[...]
    final = len(BLOCKS) - 1

    def project(i, carry):
        rows = pl.ds(pl.multiple_of(i * 128, 128), 128)

        @pl.when(i < final)
        def _():
            x_copy(i, rows).wait()

        @pl.when(i == final)
        def _():
            x_copy(final).wait()

        x = x_buf[rows, :].astype(jnp.float32)
        sq = jnp.sum(x * x, axis=1, keepdims=True)
        g_buf[rows, :] = (x * gain).astype(jnp.bfloat16)

        @pl.when(i == 0)
        def _():
            for j in range(W_PARTS):
                w_copy(j).wait()

        partial = dot(g_buf[rows, :], w_buf[...], 1, 0)
        p_own[rows, :] = partial
        p_send[rows, :] = partial.astype(jnp.bfloat16)
        sq_send[i] = jnp.transpose(jnp.broadcast_to(sq, (128, HD)))[:8, :]

        @pl.when(i == 0)
        def _():
            pl.semaphore_wait(barrier, 1 + len(senders))

        @pl.when(i < final)
        def _():
            p_copy(i, rows).start()

        @pl.when(i == final)
        def _():
            p_copy(final).start()

        sq_copy(i).start()
        return carry

    lax.fori_loop(0, len(BLOCKS), project, 0)

    cot_copy.wait()
    table_copy.wait()
    cot_buf[pl.ds(TOK, PAD - TOK), :] = tail
    lane = lax.broadcasted_iota(jnp.int32, (64, HD), 1)
    sign = jnp.where(lane < HD // 2, -1.0, 1.0)
    cos_fine = table_buf[pl.ds(16, 64), :]
    sin_fine = table_buf[pl.ds(80, 64), :]

    def tables(a, carry):
        rows = pl.ds(pl.multiple_of(a * 64, 64), 64)
        cos_coarse = table_buf[pl.ds(a, 1), :]
        sin_coarse = table_buf[pl.ds(8 + a, 1), :]
        cos_buf[rows, :] = cos_coarse * cos_fine - sin_coarse * sin_fine
        sin_buf[rows, :] = (sin_coarse * cos_fine + cos_coarse * sin_fine) * sign
        return carry

    lax.fori_loop(0, TOK // 64, tables, 0)

    def turn(c, carry):
        cols = pl.ds(pl.multiple_of(c * 256, 256), 256)
        gt_buf[cols, :] = jnp.transpose(g_buf[:, cols])
        return carry

    lax.fori_loop(0, FEAT // 256, turn, 0)

    def products(c, carry):
        rows = pl.ds(pl.multiple_of(c * 128, 128), 128)
        gram = dot(g_buf[rows, :], gt_buf[...], 1, 0)
        for level in range(3):
            short = gram.astype(jnp.bfloat16)
            gram_buf[rows, pl.ds(level * PAD, PAD)] = short
            gram = gram - short.astype(jnp.float32)
        return carry

    lax.fori_loop(0, PAD // 128, products, 0)

    dk_acc[...] = jnp.zeros_like(dk_acc)
    dv_acc[...] = jnp.zeros_like(dv_acc)
    factor = 1.0 / math.sqrt(HD)

    def put_slope(at, height, which, value):
        short = value.astype(jnp.bfloat16)
        for n in range(3):
            slope_buf[pl.ds(n * PAD + at, height), pl.ds(which * HD, HD)] = short

    for b, (at, height) in enumerate(BLOCKS):
        rows = pl.ds(at, height)
        sq_copy(b).wait()
        squares = jnp.transpose(
            jnp.broadcast_to((sq_send[b] + sq_recv[b])[0:1, :], (HD, HD))
        )
        inv = lax.rsqrt(squares[:height, :] / D + norm_eps)
        sq_own[rows, :] = inv
        scale = inv * (1.0 / math.sqrt(D))
        cos = cos_buf[rows, :]
        sin = sin_buf[rows, :]
        p_copy(b).wait()
        if early and b == final - 1:
            early_copy(0).start()

        def part(n):
            cols = pl.ds(n * HD, HD)
            return (p_own[rows, cols] + p_recv[rows, cols].astype(jnp.float32)) * scale

        q, k, v = part(0), part(1), part(2)
        q = (q * cos + pltpu.roll(q, HD // 2, 1) * sin).astype(jnp.bfloat16)
        k_buf[rows, :] = (k * cos + pltpu.roll(k, HD // 2, 1) * sin).astype(jnp.bfloat16)
        v_buf[rows, :] = v.astype(jnp.bfloat16)

        width = 128 * (b + 1)
        keys = pl.ds(0, width)
        cot = cot_buf[rows, :]
        k = k_buf[keys, :]
        v = v_buf[keys, :]
        scores = dot(q, k, 1, 1) * factor
        row = lax.broadcasted_iota(jnp.int32, (height, width), 0) + at
        col = lax.broadcasted_iota(jnp.int32, (height, width), 1)
        causal = col <= row
        scores = jnp.where(causal, scores, -1e30)
        peak = jnp.max(scores, axis=1, keepdims=True)
        lifted = jnp.where(causal, jnp.exp(scores - peak), 0.0)
        probs = lifted / jnp.sum(lifted, axis=1, keepdims=True)
        probs_low = probs.astype(jnp.bfloat16)
        dprobs = dot(cot, v, 1, 1)
        row_dots = jnp.sum(probs_low.astype(jnp.float32) * dprobs, axis=1, keepdims=True)
        dscores = (probs * (dprobs - row_dots) * factor).astype(jnp.bfloat16)
        dq = dot(dscores, k, 1, 0)
        dk_acc[keys, :] += dot(dscores, q, 0, 0)
        dv_acc[keys, :] += dot(probs_low, cot, 0, 0)
        turned = dq * cos - pltpu.roll(dq, HD // 2, 1) * sin
        put_slope(at, height, 0, turned * inv)
    every = pl.ds(0, TOK)
    cos = cos_buf[every, :]
    sin = sin_buf[every, :]
    inv = sq_own[every, :]
    dk = dk_acc[every, :]
    turned = dk * cos - pltpu.roll(dk, HD // 2, 1) * sin
    put_slope(0, TOK, 1, turned * inv)
    put_slope(0, TOK, 2, dv_acc[every, :] * inv)
    if early:
        block = dot(gt_buf[late, :], slope_buf[pl.ds(0, PAD), :], 1, 0)
        short_buf[...] = block.astype(jnp.bfloat16)
        early_copy(1).start()

    def norms(c, so_far):
        rows = pl.ds(pl.multiple_of(c * 256, 256), 256)
        image = dot(gram_buf[rows, :], slope_buf[...], 1, 0)
        image = image * slope_buf[rows, :].astype(jnp.float32)
        return so_far + jnp.sum(image.reshape(32, 8, COLS), axis=0)

    total_of = lax.fori_loop(0, PAD // 256, norms, jnp.zeros((8, COLS), jnp.float32))
    tot_send[...] = jnp.broadcast_to(jnp.sum(total_of), (8, HD))
    tot_copy.start()

    def gradient(c, carry):
        rows = pl.ds(pl.multiple_of(c * 256, 256), 256)
        grad_buf[rows, :] = dot(gt_buf[rows, :], slope_buf[pl.ds(0, PAD), :], 1, 0)
        return carry

    lax.fori_loop(0, FEAT // 256, gradient, 0)
    tot_copy.wait()
    total = jnp.maximum(tot_send[...] + tot_recv[...], 0.0)[0:1, 0:1]
    pace = rate / jnp.sqrt(total / (D * COLS) + step_eps)
    if early:
        pace_send[...] = jnp.broadcast_to(pace, (8, HD))
        early_copy(2).start()

    def step(i):
        rows = pl.ds(pl.multiple_of(i * rows_of, rows_of), rows_of)
        stepped = w_buf[rows, :].astype(jnp.float32) - grad_buf[rows, :] * pace
        step_buf[rows, :] = stepped.astype(jnp.bfloat16)

    def leg_copy(leg, i):
        rows = pl.ds(pl.multiple_of(i * rows_of, rows_of), rows_of)
        first, closing = leg == 0, leg == legs - 1
        return pltpu.make_async_remote_copy(
            src_ref=step_buf.at[rows] if first else relay_buf.at[leg - 1, rows],
            dst_ref=part_buf.at[rows] if closing else relay_buf.at[leg, rows],
            send_sem=leg_send_sems.at[leg, i],
            recv_sem=g_recv_sems.at[i] if closing else leg_recv_sems.at[leg, i],
            device_id={"node": last if closing else onward},
            device_id_type=MESH,
        )

    def send_round(i, carry):
        step(i)
        leg_copy(0, i).start()
        return carry

    def send(i, carry):
        step(i)
        g_copy(i).start()
        return carry

    if detour:
        lax.fori_loop(0, detour, send_round, 0)
    lax.fori_loop(detour, regular, send, 0)

    for leg in range(1, legs):

        def relay(i, carry, leg=leg):
            leg_copy(leg - 1, i).wait_recv()
            leg_copy(leg, i).start()
            return carry

        lax.fori_loop(0, detour, relay, 0)

    def receive(i, carry):
        rows = pl.ds(pl.multiple_of(i * rows_of, rows_of), rows_of)
        g_copy(i).wait_recv()
        mean = (step_buf[rows, :].astype(jnp.float32) + part_buf[rows, :].astype(jnp.float32)) * 0.5
        out_ref[0, rows, :] = mean.astype(jnp.bfloat16)
        return carry

    if early:
        for n in range(3):
            early_copy(n).wait()
        own = w_buf[late, :].astype(jnp.float32) - grad_buf[late, :] * pace
        theirs = old_buf[...].astype(jnp.float32) - slant_buf[...].astype(jnp.float32) * pace_recv[0:1, 0:1]
        own, theirs = (side.astype(jnp.bfloat16).astype(jnp.float32) for side in (own, theirs))
        out_ref[0, late, :] = ((own + theirs) * 0.5).astype(jnp.bfloat16)
    lax.fori_loop(detour, regular, receive, 0)
    if detour:
        lax.fori_loop(0, detour, receive, 0)

    def finish(i, carry):
        g_copy(i).wait_send()
        return carry

    lax.fori_loop(detour, regular, finish, 0)
    for leg in range(legs if detour else 0):

        def finish_leg(i, carry, leg=leg):
            leg_copy(leg, i).wait_send()
            return carry

        lax.fori_loop(0, detour, finish_leg, 0)


def round_call(level, nodes):
    bf16, f32 = jnp.bfloat16, jnp.float32
    route = route_of(level, nodes)
    chunks, early, detour, legs = route[:4]
    fresh = max(early, 1) * FEAT // chunks
    vmem, dma = pltpu.VMEM, pltpu.SemaphoreType.DMA
    return pl.pallas_call(
        functools.partial(kernel, 1 << level, nodes, route),
        out_shape=jax.ShapeDtypeStruct((1, FEAT, COLS), bf16),
        in_specs=[pl.BlockSpec(memory_space=pl.ANY)] * 5,
        out_specs=pl.BlockSpec(memory_space=pltpu.VMEM),
        scratch_shapes=[
            vmem((PAD, FEAT), bf16),
            vmem((FEAT, COLS), bf16),
            vmem((1, FEAT), f32),
            vmem((PAD, HD), bf16),
            vmem((144, HD), f32),
            vmem((TOK, HD), f32),
            vmem((TOK, HD), f32),
            vmem((PAD, FEAT), bf16),
            vmem((FEAT, PAD), bf16),
            vmem((PAD, COLS), f32),
            vmem((PAD, COLS), bf16),
            vmem((PAD, COLS), bf16),
            vmem((PAD, HD), f32),
            vmem((len(BLOCKS), 8, HD), f32),
            vmem((len(BLOCKS), 8, HD), f32),
            vmem((PAD, 3 * PAD), bf16),
            vmem((PAD, HD), bf16),
            vmem((PAD, HD), bf16),
            vmem((PAD, HD), f32),
            vmem((PAD, HD), f32),
            vmem((3 * PAD, COLS), bf16),
            vmem((FEAT, COLS), f32),
            vmem((FEAT, COLS), bf16),
            vmem((FEAT, COLS), bf16),
            vmem((8, HD), f32),
            vmem((8, HD), f32),
            dma((3,)),
            dma((len(BLOCKS),)),
            dma((W_PARTS,)),
            dma((len(BLOCKS),)),
            dma((len(BLOCKS),)),
            dma((2, len(BLOCKS))),
            dma((2,)),
            dma((chunks,)),
            dma((chunks,)),
            vmem((max(legs - 1, 1), max(detour, 1) * FEAT // chunks, COLS), bf16),
            dma((legs, max(detour, 1))),
            dma((max(legs - 1, 1), max(detour, 1))),
            vmem((fresh, COLS), bf16),
            vmem((fresh, COLS), bf16),
            vmem((fresh, COLS), bf16),
            vmem((8, HD), f32),
            vmem((8, HD), f32),
            dma((2, 3)),
        ],
        compiler_params=pltpu.CompilerParams(
            collective_id=level, has_side_effects=True, vmem_limit_bytes=40 << 20
        ),
        name=f"round_{level}",
    )


def per_device(states, weights, norm_gain, cotangent, round_index):
    nodes = lax.axis_size("node")
    levels = nodes.bit_length() - 1
    exponent = round_index[0] % levels
    table = jnp.asarray(angle_tables())
    return lax.switch(
        exponent,
        [round_call(level, nodes) for level in range(levels)],
        states,
        weights,
        norm_gain.reshape(1, FEAT),
        cotangent,
        table,
    )


def solution(mesh):
    return jax.shard_map(
        per_device,
        mesh=mesh,
        in_specs=(
            P("node", None, "tp"),
            P("node", "tp", None),
            P("tp"),
            P("node", None, None),
            P(),
        ),
        out_specs=P("node", "tp", None),
        check_vma=False,
    )
```
